32 devices in a mesh: row: 4 (over z), col: 8 (over y, x, core).
Axes of the slice: x: 2, y: 2, z: 4, core: 2. Of those that a mesh axis runs over, the one named last changes fastest.
Arguments:
- block_values: float32 [65536, 128], P(('row', 'col')), may hold values from -6 to 6
- block_owner: int32 [65536, 1], P(('row', 'col')), may hold values from 0 to 31; in each aligned block of 2048 rows (0 to 2047, 2048 to 4095, ...) at most 128 rows name the same one
- block_offset: int32 [65536], P(('row', 'col')), may hold values from 0 to 39
- block_tiles: int32 [65536], P(('row', 'col')), may hold values from 0 to 107
Outputs:
- summed: float32 [1280, 13824], P(('row', 'col'))
- occupancy: int32 [10, 108], replicated
The draws below stay inside these ranges and needn't reach their ends.
Inputs may be any that keep to these rules, and one draw needn't show every extreme that they name: `block_owner`: among the rows of one device no owner is named more than 128 times, a bound that some block reaches.
All inputs are finite; a program needn't handle non-finite values.
Results may differ from the reference program's by a relative error of at most 0.0003.
Values sent between devices are 32-bit elements; how exact they have to be, the bound alone decides.
A program may use at most 64 MiB of HBM per device.

```python
import math
import jax
import jax.numpy as jnp
import numpy as np

F = 13824
TILE = 128
ROWS_DEV = 40
KB = 2048
ROWS = 1280
CT = 108
CAP = 128
BLOCKS = 65536
DEVICES = 32


def place_ends(entries, key, least, high):
    index_at = [jax.random.randint(jax.random.fold_in(key, axis), (), 0, length) for axis, length in enumerate(entries.shape)]
    longest = entries.shape.index(max(entries.shape))
    neighbour = index_at[:longest] + [(index_at[longest] + 1) % entries.shape[longest]] + index_at[longest + 1:]
    return entries.at[tuple(index_at)].set(least).at[tuple(neighbour)].set(high)


def shard_levels(key, extent, shards, low, top_value):
    def one(axis_at, blocks):
        draws = jax.random.uniform(jax.random.fold_in(jax.random.fold_in(key, 6), axis_at), (blocks,), jnp.float32, low / len(shards), top_value / len(shards))
        return jnp.repeat(jnp.exp(draws), extent[axis_at] // blocks).reshape((-1,) + (1,) * (len(extent) - axis_at - 1))

    factor_of = one(*shards[0])
    for cut in shards[1:]:
        factor_of = factor_of * one(*cut)
    return factor_of


def routed_block(key, own, number, rows, amount, top, reach, skew):
    order = jax.random.permutation(key, amount)
    packed, usual = load_shares(amount, rows * top, reach, skew, True), load_shares(amount, rows * top, reach, skew, False)
    places = jnp.arange(amount)

    def named(sizes, offset_by):
        used = int((sizes > 0).sum())
        fixed = max(1, used // 4)
        passed = fixed + (places - fixed + offset_by * (used - fixed)) % max(1, amount - fixed)
        return jnp.zeros((amount,), jnp.int32).at[order[jnp.where(places < fixed, places, passed)]].set(jnp.asarray(sizes, jnp.int32))

    sizes = jnp.where(number % 4 == 0, named(packed, number // 4), named(usual, number - number // 4 - 1))
    mixed = jax.random.permutation(jax.random.fold_in(own, 3), amount)
    giver, sink = mixed[0:amount // 2 * 2:2], mixed[1:amount // 2 * 2:2]
    margin = jnp.minimum(sizes[giver] - 1, reach - sizes[sink]) // 2
    margin = jnp.where((giver == order[0]) | (sink == order[0]) | (sizes[sink] == 0), 0, jnp.maximum(margin, 0))
    passed = jax.random.randint(jax.random.fold_in(own, 4), (amount // 2,), 0, 1 << 20) % (margin + 1)
    sizes = sizes.at[giver].add(-passed).at[sink].add(passed)
    labels = jnp.searchsorted(jnp.cumsum(sizes), jnp.arange(rows * top), side="right").astype(jnp.int32)
    table = labels.reshape(top, rows).T
    table = table[jax.random.permutation(jax.random.fold_in(own, 1), rows)]
    offset_by = jax.random.randint(jax.random.fold_in(own, 2), (rows, 1), 0, top)
    return jnp.take_along_axis(table, (jnp.arange(top)[None, :] + offset_by) % top, axis=1)


def load_shares(number_of, total, most, lean, full):
    portions = [(1 << 20) // math.isqrt(standing ** lean) + 1 for standing in range(1, number_of + 1)]
    largest = most if full else min(most, max(-(-total // number_of), total * portions[0] // sum(portions)))
    least = 1 if total - largest >= number_of - 1 else 0
    counts, spare = [largest] + [least] * (number_of - 1), total - largest - least * (number_of - 1)
    while spare > 0:
        candidates = [i for i in range(1, number_of) if counts[i] < largest] or [i for i in range(1, number_of) if counts[i] < most]
        mass, remaining = sum([portions[i] for i in candidates]), spare
        for i in candidates:
            more = min(most - counts[i], max(1, remaining * portions[i] // mass), spare)
            counts[i] = counts[i] + more
            spare = spare - more
    return np.array(counts)


def normal_values(own_key, shape, spread, bound, pieces=(), dtype=jnp.bfloat16):
    entries = jax.random.normal(own_key, shape, jnp.float32) * spread
    if len(pieces) > 0:
        entries = shard_levels(own_key, shape, pieces, -0.22, 0.18) * entries
    return jnp.clip(entries, min=-bound, max=bound).astype(dtype)


def setup_inputs(seed: int = 0) -> dict:
    arg_keys = jax.random.split(jax.random.key(seed), 5)
    block_values = normal_values(arg_keys[0], (BLOCKS, TILE), 1.0, 6.0, ((0, 32),), jnp.float32)
    block_owner_keys = jax.random.split(jax.random.fold_in(arg_keys[1], 1), BLOCKS // KB)
    block_owner_turns = jax.random.permutation(jax.random.fold_in(arg_keys[1], 3), BLOCKS // KB)
    block_owner = jax.vmap(lambda own, number: routed_block(jax.random.fold_in(arg_keys[1], 2), own, number, KB, DEVICES, 1, CAP, 2))(block_owner_keys, block_owner_turns).reshape((BLOCKS, 1))
    block_offset = place_ends(jax.random.randint(arg_keys[2], (BLOCKS,), 0, ROWS_DEV), jax.random.fold_in(arg_keys[2], 1), 0, ROWS_DEV - 1).astype(jnp.int32)
    block_tiles = place_ends(jax.random.randint(arg_keys[3], (BLOCKS,), 0, CT), jax.random.fold_in(arg_keys[3], 1), 0, CT - 1).astype(jnp.int32)
    return {"block_values": block_values, "block_owner": block_owner, "block_offset": block_offset, "block_tiles": block_tiles}


def reference(block_values, block_owner, block_offset, block_tiles):
    tiles_count = F // TILE
    block_row = (block_owner[:, 0] * ROWS_DEV + block_offset).astype(jnp.int32)
    keys = (block_row * tiles_count + block_tiles).astype(jnp.int32)
    dense = jax.ops.segment_sum(block_values.astype(jnp.float32), keys, num_segments=ROWS * tiles_count)
    summed = dense.reshape(ROWS, F)
    count_keys = ((block_row // TILE) * tiles_count + block_tiles).astype(jnp.int32)
    ones = jnp.ones(block_row.shape, jnp.int32)
    counted = jax.ops.segment_sum(ones, count_keys, num_segments=(ROWS // TILE) * tiles_count)
    return summed, counted.reshape(ROWS // TILE, tiles_count).astype(jnp.int32)
```

```python
import functools
import math

import jax
import jax.numpy as jnp
from jax import lax
from jax.experimental import pallas as pl
from jax.experimental.pallas import tpu as pltpu
from jax.sharding import PartitionSpec as P

F = 13824
TILE = 128
ROWS_DEV = 40
SUB = 8
MESH = pl.DeviceIdType.MESH
CHAINS = 4


def spread_kernel(capacity, target_ref, key_ref, fill_ref, values_ref, send_ref, keys_ref, sem):
    fill = pltpu.make_async_copy(fill_ref, keys_ref, sem)
    fill.start()
    fill.wait()
    step = math.gcd(values_ref.shape[0], 16)

    def group(g, carry):
        base = pl.multiple_of(g * step, step)
        for i in range(step):
            t = target_ref[base + i]
            send_ref[pl.ds(t, 1), :] = values_ref[pl.ds(base + i, 1), :]
            keys_ref[t // capacity, 0, t % capacity] = key_ref[base + i]
        return carry

    lax.fori_loop(0, values_ref.shape[0] // step, group, 0)


def exchange_kernel(
    rows,
    cols,
    send_ref,
    keys_ref,
    counts_ref,
    got_ref,
    got_keys_ref,
    total_ref,
    plane,
    every,
    own,
    val_send,
    val_recv,
    key_send,
    key_recv,
    plane_send,
    plane_recv,
    every_send,
    every_recv,
    local_sem,
):
    r, c = lax.axis_index("row"), lax.axis_index("col")
    me = r * cols + c
    n = rows * cols
    barrier = pltpu.get_barrier_semaphore()

    def greet(k, carry):
        to = lax.rem(me + k, n)
        pl.semaphore_signal(
            barrier, inc=1, device_id=(to // cols, lax.rem(to, cols)), device_id_type=MESH
        )
        return carry

    lax.fori_loop(1, n, greet, 0)
    pl.semaphore_wait(barrier, n - 1)

    def plane_copy(k):
        return pltpu.make_async_remote_copy(
            src_ref=counts_ref,
            dst_ref=plane.at[r],
            send_sem=plane_send.at[k],
            recv_sem=plane_recv.at[k],
            device_id=(lax.rem(r + k, rows), c),
            device_id_type=MESH,
        )

    def every_copy(k):
        return pltpu.make_async_remote_copy(
            src_ref=plane,
            dst_ref=every.at[c],
            send_sem=every_send.at[k],
            recv_sem=every_recv.at[k],
            device_id=(r, lax.rem(c + k, cols)),
            device_id_type=MESH,
        )

    def value_copies(k):
        to_row, to_col = lax.rem(r + k // cols, rows), lax.rem(c + lax.rem(k, cols), cols)
        to = to_row * cols + to_col
        where = dict(device_id=(to_row, to_col), device_id_type=MESH)
        return (
            pltpu.make_async_remote_copy(
                src_ref=keys_ref.at[to],
                dst_ref=got_keys_ref.at[me],
                send_sem=key_send.at[k],
                recv_sem=key_recv.at[k],
                **where,
            ),
            pltpu.make_async_remote_copy(
                src_ref=send_ref.at[to],
                dst_ref=got_ref.at[me],
                send_sem=val_send.at[k],
                recv_sem=val_recv.at[k],
                **where,
            ),
        )

    for k in range(1, rows):
        plane_copy(k).start()

    def start_all(low, high):
        def one(k, carry):
            for copy in value_copies(k):
                copy.start()
            return carry

        lax.fori_loop(low, high, one, 0)

    order = sorted(range(rows), key=lambda d: -min(d, rows - d))
    for d in order:
        start_all(max(d * cols, 1), (d + 1) * cols)
    own_in = pltpu.make_async_copy(send_ref.at[me], own, local_sem.at[0])
    own_in.start()
    own_keys = pltpu.make_async_copy(keys_ref.at[me], got_keys_ref.at[me], local_sem.at[1])
    own_keys.start()
    own_counts = pltpu.make_async_copy(counts_ref, plane.at[r], local_sem.at[2])
    own_counts.start()
    own_in.wait()
    own_out = pltpu.make_async_copy(own, got_ref.at[me], local_sem.at[0])
    own_out.start()
    own_counts.wait()
    for k in range(1, rows):
        plane_copy(k).wait()

    def start_every(k, carry):
        every_copy(k).start()
        return carry

    lax.fori_loop(1, cols, start_every, 0)
    own_keys.wait()
    own_out.wait()

    def wait_all(k, carry):
        for copy in value_copies(k):
            copy.wait()
        return carry

    lax.fori_loop(1, n, wait_all, 0)

    def wait_every(k, carry):
        every_copy(k).wait()
        return carry

    lax.fori_loop(1, cols, wait_every, 0)
    mine = plane[0]
    for i in range(1, rows):
        mine = mine + plane[i]
    total_ref[...] = mine

    def add_every(k, carry):
        other = lax.rem(c + k, cols)
        for i in range(rows):
            total_ref[...] += every[other, i]
        return carry

    lax.fori_loop(1, cols, add_every, 0)


def place_kernel(keys_ref, values_ref, out_ref, *rest):
    accs, (outbuf, sems) = rest[:CHAINS], rest[CHAINS:]
    step = pl.program_id(0)
    sources, _, capacity = keys_ref.shape
    cells = accs[0].shape[0] - SUB
    tiles = cells // ROWS_DEV
    unit = math.gcd(capacity, 32)

    @pl.when(step == 0)
    def _():
        for acc in accs:
            acc[...] = jnp.zeros_like(acc)

    def source(s, carry):
        def group(g, carry):
            base = pl.multiple_of(g * unit, unit)
            row = pl.multiple_of(s * capacity + base, unit)
            for j in range(0, unit, CHAINS):
                at = [keys_ref[s, 0, base + j + q] for q in range(CHAINS)]
                sums = [
                    accs[q][pl.ds(at[q], 1), :] + values_ref[pl.ds(row + j + q, 1), :]
                    for q in range(CHAINS)
                ]
                for q in range(CHAINS):
                    accs[q][pl.ds(at[q], 1), :] = sums[q]
            return carry

        return lax.fori_loop(0, capacity // unit, group, carry)

    lax.fori_loop(0, sources, source, 0)

    @pl.when(step == pl.num_programs(0) - 1)
    def _():
        copies = []
        for g in range(ROWS_DEV // SUB):
            for c in range(tiles):
                at = pl.ds((g * tiles + c) * SUB, SUB)
                total = accs[0][at, :]
                for acc in accs[1:]:
                    total = total + acc[at, :]
                outbuf[g * SUB : (g + 1) * SUB, c * TILE : (c + 1) * TILE] = total
            rows = pl.ds(g * SUB, SUB)
            copy = pltpu.make_async_copy(outbuf.at[rows], out_ref.at[rows], sems.at[g])
            copy.start()
            copies.append(copy)
        for copy in copies:
            copy.wait()


def body(block_values, block_owner, block_offset, block_tiles):
    tiles_count = F // TILE
    size_row = lax.axis_size("row")
    size_col = lax.axis_size("col")
    devices_all = size_row * size_col
    local_blocks = block_values.shape[0]
    capacity = 2 * local_blocks // devices_all
    slots_total = devices_all * capacity
    owner = block_owner[:, 0]
    cells = ROWS_DEV * tiles_count
    owner_hot = (owner[:, None] == jnp.arange(devices_all, dtype=jnp.int32)[None, :]).astype(
        jnp.bfloat16
    )
    positions = jnp.arange(local_blocks, dtype=jnp.int32)
    earlier = (positions[None, :] < positions[:, None]).astype(jnp.bfloat16)
    before = jnp.dot(earlier, owner_hot, preferred_element_type=jnp.float32)
    slot = jnp.sum(before * owner_hot.astype(jnp.float32), axis=1).astype(jnp.int32)
    target = owner * capacity + slot
    local_keys = (block_offset // SUB * tiles_count + block_tiles) * SUB + block_offset % SUB

    vmem, smem, anywhere = (
        pl.BlockSpec(memory_space=m) for m in (pltpu.VMEM, pltpu.SMEM, pl.ANY)
    )
    fill = jnp.full((devices_all, 1, capacity), cells, jnp.int32)
    send, send_keys = pl.pallas_call(
        functools.partial(spread_kernel, capacity),
        out_shape=(
            jax.ShapeDtypeStruct((slots_total, TILE), jnp.float32),
            jax.ShapeDtypeStruct((devices_all, 1, capacity), jnp.int32),
        ),
        in_specs=[smem, smem, anywhere, vmem],
        out_specs=(vmem, smem),
        scratch_shapes=[pltpu.SemaphoreType.DMA],
        name="spread",
    )(target, local_keys, fill, block_values)

    rows_total = ROWS_DEV * devices_all
    tile_rows = rows_total // TILE
    block_row = owner * ROWS_DEV + block_offset
    tile_row = block_row // TILE
    row_hot = (jnp.arange(tile_rows, dtype=jnp.int32)[:, None] == tile_row[None, :]).astype(
        jnp.bfloat16
    )
    col_hot = (jnp.arange(TILE, dtype=jnp.int32)[:, None] == block_tiles[None, :]).astype(
        jnp.bfloat16
    )
    local_counts = lax.dot_general(
        row_hot, col_hot, (((1,), (1,)), ((), ())), preferred_element_type=jnp.float32
    ).astype(jnp.int32)

    sems = pltpu.SemaphoreType.DMA
    got, got_keys, total = pl.pallas_call(
        functools.partial(exchange_kernel, size_row, size_col),
        out_shape=(
            jax.ShapeDtypeStruct((devices_all, capacity, TILE), jnp.float32),
            jax.ShapeDtypeStruct((devices_all, 1, capacity), jnp.int32),
            jax.ShapeDtypeStruct((tile_rows, TILE), jnp.int32),
        ),
        in_specs=[anywhere, anywhere, anywhere],
        out_specs=(anywhere, anywhere, vmem),
        scratch_shapes=[
            pltpu.VMEM((size_row, tile_rows, TILE), jnp.int32),
            pltpu.VMEM((size_col, size_row, tile_rows, TILE), jnp.int32),
            pltpu.VMEM((capacity, TILE), jnp.float32),
            sems((devices_all,)),
            sems((devices_all,)),
            sems((devices_all,)),
            sems((devices_all,)),
            sems((size_row,)),
            sems((size_row,)),
            sems((size_col,)),
            sems((size_col,)),
            sems((3,)),
        ],
        compiler_params=pltpu.CompilerParams(collective_id=0, has_side_effects=True),
        name="exchange",
    )(send.reshape(devices_all, capacity, TILE), send_keys, local_counts)

    batch = math.gcd(devices_all, 4)
    summed = pl.pallas_call(
        place_kernel,
        out_shape=jax.ShapeDtypeStruct((ROWS_DEV, F), jnp.float32),
        grid=(devices_all // batch,),
        in_specs=[
            pl.BlockSpec((batch, 1, capacity), lambda i: (i, 0, 0), memory_space=pltpu.SMEM),
            pl.BlockSpec((batch * capacity, TILE), lambda i: (i, 0)),
        ],
        out_specs=anywhere,
        scratch_shapes=[pltpu.VMEM((cells + SUB, TILE), jnp.float32)] * CHAINS
        + [pltpu.VMEM((ROWS_DEV, F), jnp.float32), sems((ROWS_DEV // SUB,))],
        name="place",
    )(got_keys, got.reshape(slots_total, TILE))
    return (summed, total[:, :tiles_count])


def solution(mesh):
    in_specs = (
        P(("row", "col"), None),
        P(("row", "col"), None),
        P(("row", "col")),
        P(("row", "col")),
    )
    out_specs = (P(("row", "col"), None), P())
    return jax.shard_map(body, mesh=mesh, in_specs=in_specs, out_specs=out_specs, check_vma=False)
```

```python
import functools
import math

import jax
import jax.numpy as jnp
from jax import lax
from jax.experimental import pallas as pl
from jax.experimental.pallas import tpu as pltpu
from jax.sharding import PartitionSpec as P

F = 13824
TILE = 128
ROWS_DEV = 40
SUB = 8
MESH = pl.DeviceIdType.MESH
CHAINS = 4


def spread_kernel(target_ref, key_ref, fill_ref, values_ref, send_ref, keys_ref, sem):
    fill = pltpu.make_async_copy(fill_ref, keys_ref, sem)
    fill.start()
    fill.wait()
    step = math.gcd(values_ref.shape[0], 16)

    def group(g, carry):
        base = pl.multiple_of(g * step, step)
        to = [target_ref[base + i] for i in range(step)]
        keys = [key_ref[base + i] for i in range(step)]
        for i in range(step):
            send_ref[pl.ds(to[i], 1), :] = values_ref[pl.ds(base + i, 1), :]
        for i in range(step):
            keys_ref[to[i]] = keys[i]
        return carry

    lax.fori_loop(0, values_ref.shape[0] // step, group, 0)


def exchange_kernel(
    rows,
    cols,
    send_ref,
    keys_ref,
    counts_ref,
    got_ref,
    got_keys_ref,
    total_ref,
    plane,
    every,
    own,
    val_send,
    val_recv,
    key_send,
    key_recv,
    plane_send,
    plane_recv,
    every_send,
    every_recv,
    local_sem,
):
    r, c = lax.axis_index("row"), lax.axis_index("col")
    me = r * cols + c
    n = rows * cols
    barrier = pltpu.get_barrier_semaphore()

    paired = rows & (rows - 1) == 0
    order = [rows // 2] + [d for d in range(1, rows) if d != rows // 2] + [0]

    def partner(at, d):
        if not paired:
            return lax.rem(at + d, rows)
        out, bit = at, 1
        while bit < rows:
            if d & bit:
                half = lax.rem(out // bit, 2)
                out = out + bit - 2 * bit * half
            bit *= 2
        return out

    def greet(k, carry):
        to = lax.rem(me + k, n)
        pl.semaphore_signal(
            barrier, inc=1, device_id=(to // cols, lax.rem(to, cols)), device_id_type=MESH
        )
        return carry

    lax.fori_loop(1, n, greet, 0)
    pl.semaphore_wait(barrier, n - 1)

    def plane_copy(k):
        return pltpu.make_async_remote_copy(
            src_ref=counts_ref,
            dst_ref=plane.at[r],
            send_sem=plane_send.at[k],
            recv_sem=plane_recv.at[k],
            device_id=(lax.rem(r + k, rows), c),
            device_id_type=MESH,
        )

    def every_copy(k):
        return pltpu.make_async_remote_copy(
            src_ref=plane,
            dst_ref=every.at[c],
            send_sem=every_send.at[k],
            recv_sem=every_recv.at[k],
            device_id=(r, lax.rem(c + k, cols)),
            device_id_type=MESH,
        )

    def value_copies(d, e):
        k = d * cols + e
        to_row, to_col = partner(r, d), lax.rem(c + e, cols)
        to = to_row * cols + to_col
        where = dict(device_id=(to_row, to_col), device_id_type=MESH)
        return (
            pltpu.make_async_remote_copy(
                src_ref=keys_ref.at[to],
                dst_ref=got_keys_ref.at[me],
                send_sem=key_send.at[k],
                recv_sem=key_recv.at[k],
                **where,
            ),
            pltpu.make_async_remote_copy(
                src_ref=send_ref.at[to],
                dst_ref=got_ref.at[me],
                send_sem=val_send.at[k],
                recv_sem=val_recv.at[k],
                **where,
            ),
        )

    for k in range(1, rows):
        plane_copy(k).start()

    def for_all(act):
        for d in order:

            def one(e, carry):
                for copy in value_copies(d, e):
                    act(copy)
                return carry

            lax.fori_loop(0 if d else 1, cols, one, 0)

    for_all(lambda copy: copy.start())
    own_in = pltpu.make_async_copy(send_ref.at[me], own, local_sem.at[0])
    own_in.start()
    own_keys = pltpu.make_async_copy(keys_ref.at[me], got_keys_ref.at[me], local_sem.at[1])
    own_keys.start()
    own_counts = pltpu.make_async_copy(counts_ref, plane.at[r], local_sem.at[2])
    own_counts.start()
    own_in.wait()
    own_out = pltpu.make_async_copy(own, got_ref.at[me], local_sem.at[0])
    own_out.start()
    own_counts.wait()
    for k in range(1, rows):
        plane_copy(k).wait()

    def start_every(k, carry):
        every_copy(k).start()
        return carry

    lax.fori_loop(1, cols, start_every, 0)
    own_keys.wait()
    own_out.wait()

    for_all(lambda copy: copy.wait())

    def wait_every(k, carry):
        every_copy(k).wait()
        return carry

    lax.fori_loop(1, cols, wait_every, 0)
    mine = plane[0]
    for i in range(1, rows):
        mine = mine + plane[i]
    total_ref[...] = mine

    def add_every(k, carry):
        other = lax.rem(c + k, cols)
        for i in range(rows):
            total_ref[...] += every[other, i]
        return carry

    lax.fori_loop(1, cols, add_every, 0)


def place_kernel(keys_ref, values_ref, out_ref, *rest):
    accs, (outbuf, sems) = rest[:CHAINS], rest[CHAINS:]
    step = pl.program_id(0)
    sources, _, capacity = keys_ref.shape
    cells = accs[0].shape[0] - SUB
    tiles = cells // ROWS_DEV
    unit = math.gcd(capacity, 32)

    @pl.when(step == 0)
    def _():
        for acc in accs:
            acc[...] = jnp.zeros_like(acc)

    def source(s, carry):
        def group(g, carry):
            base = pl.multiple_of(g * unit, unit)
            row = pl.multiple_of(s * capacity + base, unit)
            at = [keys_ref[s, 0, base + j] for j in range(unit)]
            for j in range(0, unit, CHAINS):
                sums = [
                    accs[q][pl.ds(at[j + q], 1), :] + values_ref[pl.ds(row + j + q, 1), :]
                    for q in range(CHAINS)
                ]
                for q in range(CHAINS):
                    accs[q][pl.ds(at[j + q], 1), :] = sums[q]
            return carry

        return lax.fori_loop(0, capacity // unit, group, carry)

    lax.fori_loop(0, sources, source, 0)

    @pl.when(step == pl.num_programs(0) - 1)
    def _():
        copies = []
        for g in range(ROWS_DEV // SUB):
            for c in range(tiles):
                at = pl.ds((g * tiles + c) * SUB, SUB)
                total = accs[0][at, :]
                for acc in accs[1:]:
                    total = total + acc[at, :]
                outbuf[g * SUB : (g + 1) * SUB, c * TILE : (c + 1) * TILE] = total
            rows = pl.ds(g * SUB, SUB)
            copy = pltpu.make_async_copy(outbuf.at[rows], out_ref.at[rows], sems.at[g])
            copy.start()
            copies.append(copy)
        for copy in copies:
            copy.wait()


def body(block_values, block_owner, block_offset, block_tiles):
    tiles_count = F // TILE
    size_row = lax.axis_size("row")
    size_col = lax.axis_size("col")
    devices_all = size_row * size_col
    local_blocks = block_values.shape[0]
    capacity = 2 * local_blocks // devices_all
    slots_total = devices_all * capacity
    owner = block_owner[:, 0]
    cells = ROWS_DEV * tiles_count
    owner_hot = (owner[:, None] == jnp.arange(devices_all, dtype=jnp.int32)[None, :]).astype(
        jnp.bfloat16
    )
    positions = jnp.arange(local_blocks, dtype=jnp.int32)
    earlier = (positions[None, :] < positions[:, None]).astype(jnp.bfloat16)
    before = jnp.dot(earlier, owner_hot, preferred_element_type=jnp.float32)
    slot = jnp.sum(before * owner_hot.astype(jnp.float32), axis=1).astype(jnp.int32)
    target = owner * capacity + slot
    local_keys = (block_offset // SUB * tiles_count + block_tiles) * SUB + block_offset % SUB

    vmem, smem, anywhere = (
        pl.BlockSpec(memory_space=m) for m in (pltpu.VMEM, pltpu.SMEM, pl.ANY)
    )
    fill = jnp.full((slots_total,), cells, jnp.int32)
    send, send_keys = pl.pallas_call(
        spread_kernel,
        out_shape=(
            jax.ShapeDtypeStruct((slots_total, TILE), jnp.float32),
            jax.ShapeDtypeStruct((slots_total,), jnp.int32),
        ),
        in_specs=[smem, smem, anywhere, vmem],
        out_specs=(vmem, smem),
        scratch_shapes=[pltpu.SemaphoreType.DMA],
        name="spread",
    )(target, local_keys, fill, block_values)

    rows_total = ROWS_DEV * devices_all
    tile_rows = rows_total // TILE
    block_row = owner * ROWS_DEV + block_offset
    tile_row = block_row // TILE
    row_hot = (jnp.arange(tile_rows, dtype=jnp.int32)[:, None] == tile_row[None, :]).astype(
        jnp.bfloat16
    )
    col_hot = (jnp.arange(TILE, dtype=jnp.int32)[:, None] == block_tiles[None, :]).astype(
        jnp.bfloat16
    )
    local_counts = lax.dot_general(
        row_hot, col_hot, (((1,), (1,)), ((), ())), preferred_element_type=jnp.float32
    ).astype(jnp.int32)

    sems = pltpu.SemaphoreType.DMA
    got, got_keys, total = pl.pallas_call(
        functools.partial(exchange_kernel, size_row, size_col),
        out_shape=(
            jax.ShapeDtypeStruct((devices_all, capacity, TILE), jnp.float32),
            jax.ShapeDtypeStruct((devices_all, 1, capacity), jnp.int32),
            jax.ShapeDtypeStruct((tile_rows, TILE), jnp.int32),
        ),
        in_specs=[anywhere, anywhere, anywhere],
        out_specs=(anywhere, anywhere, vmem),
        scratch_shapes=[
            pltpu.VMEM((size_row, tile_rows, TILE), jnp.int32),
            pltpu.VMEM((size_col, size_row, tile_rows, TILE), jnp.int32),
            pltpu.VMEM((capacity, TILE), jnp.float32),
            sems((devices_all,)),
            sems((devices_all,)),
            sems((devices_all,)),
            sems((devices_all,)),
            sems((size_row,)),
            sems((size_row,)),
            sems((size_col,)),
            sems((size_col,)),
            sems((3,)),
        ],
        compiler_params=pltpu.CompilerParams(collective_id=0, has_side_effects=True),
        name="exchange",
    )(
        send.reshape(devices_all, capacity, TILE),
        send_keys.reshape(devices_all, 1, capacity),
        local_counts,
    )

    batch = math.gcd(devices_all, 4)
    summed = pl.pallas_call(
        place_kernel,
        out_shape=jax.ShapeDtypeStruct((ROWS_DEV, F), jnp.float32),
        grid=(devices_all // batch,),
        in_specs=[
            pl.BlockSpec((batch, 1, capacity), lambda i: (i, 0, 0), memory_space=pltpu.SMEM),
            pl.BlockSpec((batch * capacity, TILE), lambda i: (i, 0)),
        ],
        out_specs=anywhere,
        scratch_shapes=[pltpu.VMEM((cells + SUB, TILE), jnp.float32)] * CHAINS
        + [pltpu.VMEM((ROWS_DEV, F), jnp.float32), sems((ROWS_DEV // SUB,))],
        name="place",
    )(got_keys, got.reshape(slots_total, TILE))
    return (summed, total[:, :tiles_count])


def solution(mesh):
    in_specs = (
        P(("row", "col"), None),
        P(("row", "col"), None),
        P(("row", "col")),
        P(("row", "col")),
    )
    out_specs = (P(("row", "col"), None), P())
    return jax.shard_map(body, mesh=mesh, in_specs=in_specs, out_specs=out_specs, check_vma=False)
```

```python
import functools
import math

import jax
import jax.numpy as jnp
from jax import lax
from jax.experimental import pallas as pl
from jax.experimental.pallas import tpu as pltpu
from jax.sharding import PartitionSpec as P

F = 13824
TILE = 128
ROWS_DEV = 40
SUB = 8
MESH = pl.DeviceIdType.MESH
CHAINS = 8


def spread_kernel(target_ref, key_ref, fill_ref, values_ref, send_ref, keys_ref, sem):
    fill = pltpu.make_async_copy(fill_ref, keys_ref, sem)
    fill.start()
    fill.wait()
    step = math.gcd(values_ref.shape[0], 16)

    def group(g, carry):
        base = pl.multiple_of(g * step, step)
        to = [target_ref[base + i] for i in range(step)]
        keys = [key_ref[base + i] for i in range(step)]
        for i in range(step):
            send_ref[pl.ds(to[i], 1), :] = values_ref[pl.ds(base + i, 1), :]
        for i in range(step):
            keys_ref[to[i]] = keys[i]
        return carry

    lax.fori_loop(0, values_ref.shape[0] // step, group, 0)


def exchange_kernel(
    rows,
    cols,
    send_ref,
    keys_ref,
    counts_ref,
    got_ref,
    got_keys_ref,
    total_ref,
    plane,
    every,
    own,
    val_send,
    val_recv,
    key_send,
    key_recv,
    plane_send,
    plane_recv,
    every_send,
    every_recv,
    local_sem,
):
    r, c = lax.axis_index("row"), lax.axis_index("col")
    me = r * cols + c
    n = rows * cols
    barrier = pltpu.get_barrier_semaphore()

    paired = rows & (rows - 1) == 0
    half = rows // 2
    near, far = list(range(1, half)), list(range(half, rows))
    inside = far + near + [0]
    outside = near + [0] + far if paired else inside
    beside = ((r + 1) // half) * ((rows - r) // half) if rows > 2 else 1

    def partner(at, d):
        if not paired:
            return lax.rem(at + d, rows)
        out, bit = 0, 1
        while bit < rows:
            out = out + bit * lax.rem(at // bit + d // bit, 2)
            bit *= 2
        return out

    def greet(k, carry):
        to = lax.rem(me + k, n)
        pl.semaphore_signal(
            barrier, inc=1, device_id=(to // cols, lax.rem(to, cols)), device_id_type=MESH
        )
        return carry

    lax.fori_loop(1, n, greet, 0)
    pl.semaphore_wait(barrier, n - 1)

    def plane_copy(k):
        return pltpu.make_async_remote_copy(
            src_ref=counts_ref,
            dst_ref=plane.at[r],
            send_sem=plane_send.at[k],
            recv_sem=plane_recv.at[k],
            device_id=(lax.rem(r + k, rows), c),
            device_id_type=MESH,
        )

    def every_copy(k):
        return pltpu.make_async_remote_copy(
            src_ref=plane,
            dst_ref=every.at[c],
            send_sem=every_send.at[k],
            recv_sem=every_recv.at[k],
            device_id=(r, lax.rem(c + k, cols)),
            device_id_type=MESH,
        )

    def value_copies(d, e):
        k = d * cols + e
        to_row, to_col = partner(r, d), lax.rem(c + e, cols)
        to = to_row * cols + to_col
        where = dict(device_id=(to_row, to_col), device_id_type=MESH)
        return (
            pltpu.make_async_remote_copy(
                src_ref=keys_ref.at[to],
                dst_ref=got_keys_ref.at[me],
                send_sem=key_send.at[k],
                recv_sem=key_recv.at[k],
                **where,
            ),
            pltpu.make_async_remote_copy(
                src_ref=send_ref.at[to],
                dst_ref=got_ref.at[me],
                send_sem=val_send.at[k],
                recv_sem=val_recv.at[k],
                **where,
            ),
        )

    for k in range(1, rows):
        plane_copy(k).start()

    def for_all(act):
        for out, ins in zip(outside, inside):
            d = out + beside * (ins - out)

            def one(e, carry):
                for copy in value_copies(d, e):
                    act(copy)
                return carry

            lax.fori_loop(1 - (d + rows - 1) // rows, cols, one, 0)

    for_all(lambda copy: copy.start())
    own_in = pltpu.make_async_copy(send_ref.at[me], own, local_sem.at[0])
    own_in.start()
    own_keys = pltpu.make_async_copy(keys_ref.at[me], got_keys_ref.at[me], local_sem.at[1])
    own_keys.start()
    own_counts = pltpu.make_async_copy(counts_ref, plane.at[r], local_sem.at[2])
    own_counts.start()
    own_in.wait()
    own_out = pltpu.make_async_copy(own, got_ref.at[me], local_sem.at[0])
    own_out.start()
    own_counts.wait()
    for k in range(1, rows):
        plane_copy(k).wait()

    def start_every(k, carry):
        every_copy(k).start()
        return carry

    lax.fori_loop(1, cols, start_every, 0)
    own_keys.wait()
    own_out.wait()

    for_all(lambda copy: copy.wait())

    def wait_every(k, carry):
        every_copy(k).wait()
        return carry

    lax.fori_loop(1, cols, wait_every, 0)
    mine = plane[0]
    for i in range(1, rows):
        mine = mine + plane[i]
    total_ref[...] = mine

    def add_every(k, carry):
        other = lax.rem(c + k, cols)
        for i in range(rows):
            total_ref[...] += every[other, i]
        return carry

    lax.fori_loop(1, cols, add_every, 0)


def place_kernel(keys_ref, values_ref, out_ref, *rest):
    accs, (outbuf, sems) = rest[:CHAINS], rest[CHAINS:]
    step = pl.program_id(0)
    sources, _, capacity = keys_ref.shape
    cells = accs[0].shape[0] - SUB
    tiles = cells // ROWS_DEV

    @pl.when(step == 0)
    def _():
        for acc in accs:
            acc[...] = jnp.zeros_like(acc)

    def source(s, carry):
        row = pl.multiple_of(s * capacity, capacity)
        for j in range(0, capacity, CHAINS):
            at = [keys_ref[s, 0, j + q] for q in range(CHAINS)]
            sums = [
                accs[q][pl.ds(at[q], 1), :] + values_ref[pl.ds(row + j + q, 1), :]
                for q in range(CHAINS)
            ]
            for q in range(CHAINS):
                accs[q][pl.ds(at[q], 1), :] = sums[q]
        return carry

    lax.fori_loop(0, sources, source, 0)

    @pl.when(step == pl.num_programs(0) - 1)
    def _():
        copies = []
        for g in range(ROWS_DEV // SUB):
            for c in range(tiles):
                at = pl.ds((g * tiles + c) * SUB, SUB)
                total = accs[0][at, :]
                for acc in accs[1:]:
                    total = total + acc[at, :]
                outbuf[g * SUB : (g + 1) * SUB, c * TILE : (c + 1) * TILE] = total
            rows = pl.ds(g * SUB, SUB)
            copy = pltpu.make_async_copy(outbuf.at[rows], out_ref.at[rows], sems.at[g])
            copy.start()
            copies.append(copy)
        for copy in copies:
            copy.wait()


def body(block_values, block_owner, block_offset, block_tiles):
    tiles_count = F // TILE
    size_row = lax.axis_size("row")
    size_col = lax.axis_size("col")
    devices_all = size_row * size_col
    local_blocks = block_values.shape[0]
    capacity = 2 * local_blocks // devices_all
    slots_total = devices_all * capacity
    owner = block_owner[:, 0]
    cells = ROWS_DEV * tiles_count
    owner_hot = (owner[:, None] == jnp.arange(devices_all, dtype=jnp.int32)[None, :]).astype(
        jnp.bfloat16
    )
    positions = jnp.arange(local_blocks, dtype=jnp.int32)
    earlier = (positions[None, :] < positions[:, None]).astype(jnp.bfloat16)
    before = jnp.dot(earlier, owner_hot, preferred_element_type=jnp.float32)
    slot = jnp.sum(before * owner_hot.astype(jnp.float32), axis=1).astype(jnp.int32)
    target = owner * capacity + slot
    local_keys = (block_offset // SUB * tiles_count + block_tiles) * SUB + block_offset % SUB

    vmem, smem, anywhere = (
        pl.BlockSpec(memory_space=m) for m in (pltpu.VMEM, pltpu.SMEM, pl.ANY)
    )
    fill = jnp.full((slots_total,), cells, jnp.int32)
    send, send_keys = pl.pallas_call(
        spread_kernel,
        out_shape=(
            jax.ShapeDtypeStruct((slots_total, TILE), jnp.float32),
            jax.ShapeDtypeStruct((slots_total,), jnp.int32),
        ),
        in_specs=[smem, smem, anywhere, vmem],
        out_specs=(vmem, smem),
        scratch_shapes=[pltpu.SemaphoreType.DMA],
        name="spread",
    )(target, local_keys, fill, block_values)

    rows_total = ROWS_DEV * devices_all
    tile_rows = rows_total // TILE
    block_row = owner * ROWS_DEV + block_offset
    tile_row = block_row // TILE
    row_hot = (jnp.arange(tile_rows, dtype=jnp.int32)[:, None] == tile_row[None, :]).astype(
        jnp.bfloat16
    )
    col_hot = (jnp.arange(TILE, dtype=jnp.int32)[:, None] == block_tiles[None, :]).astype(
        jnp.bfloat16
    )
    local_counts = lax.dot_general(
        row_hot, col_hot, (((1,), (1,)), ((), ())), preferred_element_type=jnp.float32
    ).astype(jnp.int32)

    sems = pltpu.SemaphoreType.DMA
    got, got_keys, total = pl.pallas_call(
        functools.partial(exchange_kernel, size_row, size_col),
        out_shape=(
            jax.ShapeDtypeStruct((devices_all, capacity, TILE), jnp.float32),
            jax.ShapeDtypeStruct((devices_all, 1, capacity), jnp.int32),
            jax.ShapeDtypeStruct((tile_rows, TILE), jnp.int32),
        ),
        in_specs=[anywhere, anywhere, anywhere],
        out_specs=(anywhere, anywhere, vmem),
        scratch_shapes=[
            pltpu.VMEM((size_row, tile_rows, TILE), jnp.int32),
            pltpu.VMEM((size_col, size_row, tile_rows, TILE), jnp.int32),
            pltpu.VMEM((capacity, TILE), jnp.float32),
            sems((devices_all,)),
            sems((devices_all,)),
            sems((devices_all,)),
            sems((devices_all,)),
            sems((size_row,)),
            sems((size_row,)),
            sems((size_col,)),
            sems((size_col,)),
            sems((3,)),
        ],
        compiler_params=pltpu.CompilerParams(collective_id=0, has_side_effects=True),
        name="exchange",
    )(
        send.reshape(devices_all, capacity, TILE),
        send_keys.reshape(devices_all, 1, capacity),
        local_counts,
    )

    batch = math.gcd(devices_all, 4)
    summed = pl.pallas_call(
        place_kernel,
        out_shape=jax.ShapeDtypeStruct((ROWS_DEV, F), jnp.float32),
        grid=(devices_all // batch,),
        in_specs=[
            pl.BlockSpec((batch, 1, capacity), lambda i: (i, 0, 0), memory_space=pltpu.SMEM),
            pl.BlockSpec((batch * capacity, TILE), lambda i: (i, 0)),
        ],
        out_specs=anywhere,
        scratch_shapes=[pltpu.VMEM((cells + SUB, TILE), jnp.float32)] * CHAINS
        + [pltpu.VMEM((ROWS_DEV, F), jnp.float32), sems((ROWS_DEV // SUB,))],
        name="place",
    )(got_keys, got.reshape(slots_total, TILE))
    return (summed, total[:, :tiles_count])


def solution(mesh):
    in_specs = (
        P(("row", "col"), None),
        P(("row", "col"), None),
        P(("row", "col")),
        P(("row", "col")),
    )
    out_specs = (P(("row", "col"), None), P())
    return jax.shard_map(body, mesh=mesh, in_specs=in_specs, out_specs=out_specs, check_vma=False)
```

```python
import functools
import math

import jax
import jax.numpy as jnp
from jax import lax
from jax.experimental import pallas as pl
from jax.experimental.pallas import tpu as pltpu
from jax.sharding import PartitionSpec as P

F = 13824
TILE = 128
ROWS_DEV = 40
SUB = 8
MESH = pl.DeviceIdType.MESH
CHAINS = 8


def spread_kernel(target_ref, key_ref, fill_ref, values_ref, send_ref, keys_ref, sem):
    fill = pltpu.make_async_copy(fill_ref, keys_ref, sem)
    fill.start()
    fill.wait()
    step, part = math.gcd(values_ref.shape[0], 128), math.gcd(values_ref.shape[0], 16)

    def group(g, carry):
        base = pl.multiple_of(g * step, step)
        for j in range(0, step, part):
            spots = range(j, j + part)
            to = [target_ref[base + i] for i in spots]
            keys = [key_ref[base + i] for i in spots]
            for i in spots:
                send_ref[pl.ds(to[i - j], 1), :] = values_ref[pl.ds(base + i, 1), :]
            for i in spots:
                keys_ref[to[i - j]] = keys[i - j]
        return carry

    lax.fori_loop(0, values_ref.shape[0] // step, group, 0)


def exchange_kernel(
    rows,
    cols,
    send_ref,
    keys_ref,
    counts_ref,
    got_ref,
    got_keys_ref,
    total_ref,
    plane,
    every,
    own,
    val_send,
    val_recv,
    key_send,
    key_recv,
    plane_send,
    plane_recv,
    every_send,
    every_recv,
    local_sem,
):
    r, c = lax.axis_index("row"), lax.axis_index("col")
    me = r * cols + c
    n = rows * cols
    barrier = pltpu.get_barrier_semaphore()

    paired = rows & (rows - 1) == 0
    half = rows // 2
    near, far = list(range(1, half)), list(range(half, rows))
    inside = far + near + [0]
    outside = near + [0] + far if paired else inside
    beside = ((r + 1) // half) * ((rows - r) // half) if rows > 2 else 1

    def partner(at, d):
        if not paired:
            return lax.rem(at + d, rows)
        out, bit = 0, 1
        while bit < rows:
            out = out + bit * lax.rem(at // bit + d // bit, 2)
            bit *= 2
        return out

    def greet(k, carry):
        to = lax.rem(me + k, n)
        pl.semaphore_signal(
            barrier, inc=1, device_id=(to // cols, lax.rem(to, cols)), device_id_type=MESH
        )
        return carry

    lax.fori_loop(1, n, greet, 0)
    pl.semaphore_wait(barrier, n - 1)

    def plane_copy(k):
        return pltpu.make_async_remote_copy(
            src_ref=counts_ref,
            dst_ref=plane.at[r],
            send_sem=plane_send.at[k],
            recv_sem=plane_recv.at[k],
            device_id=(lax.rem(r + k, rows), c),
            device_id_type=MESH,
        )

    def every_copy(k):
        return pltpu.make_async_remote_copy(
            src_ref=plane,
            dst_ref=every.at[c],
            send_sem=every_send.at[k],
            recv_sem=every_recv.at[k],
            device_id=(r, lax.rem(c + k, cols)),
            device_id_type=MESH,
        )

    def value_copies(d, e):
        k = d * cols + e
        to_row, to_col = partner(r, d), lax.rem(c + e, cols)
        to = to_row * cols + to_col
        where = dict(device_id=(to_row, to_col), device_id_type=MESH)
        return (
            pltpu.make_async_remote_copy(
                src_ref=keys_ref.at[to],
                dst_ref=got_keys_ref.at[me],
                send_sem=key_send.at[k],
                recv_sem=key_recv.at[k],
                **where,
            ),
            pltpu.make_async_remote_copy(
                src_ref=send_ref.at[to],
                dst_ref=got_ref.at[me],
                send_sem=val_send.at[k],
                recv_sem=val_recv.at[k],
                **where,
            ),
        )

    for k in range(1, rows):
        plane_copy(k).start()

    def for_all(act):
        for out, ins in zip(outside, inside):
            d = out + beside * (ins - out)

            def one(e, carry):
                for copy in value_copies(d, e):
                    act(copy)
                return carry

            lax.fori_loop(1 - (d + rows - 1) // rows, cols, one, 0)

    for_all(lambda copy: copy.start())
    own_in = pltpu.make_async_copy(send_ref.at[me], own, local_sem.at[0])
    own_in.start()
    own_keys = pltpu.make_async_copy(keys_ref.at[me], got_keys_ref.at[me], local_sem.at[1])
    own_keys.start()
    own_counts = pltpu.make_async_copy(counts_ref, plane.at[r], local_sem.at[2])
    own_counts.start()
    own_in.wait()
    own_out = pltpu.make_async_copy(own, got_ref.at[me], local_sem.at[0])
    own_out.start()
    own_counts.wait()
    for k in range(1, rows):
        plane_copy(k).wait()

    def start_every(k, carry):
        every_copy(k).start()
        return carry

    lax.fori_loop(1, cols, start_every, 0)
    own_keys.wait()
    own_out.wait()

    for_all(lambda copy: copy.wait())

    def wait_every(k, carry):
        every_copy(k).wait()
        return carry

    lax.fori_loop(1, cols, wait_every, 0)
    mine = plane[0]
    for i in range(1, rows):
        mine = mine + plane[i]
    total_ref[...] = mine

    def add_every(k, carry):
        other = lax.rem(c + k, cols)
        for i in range(rows):
            total_ref[...] += every[other, i]
        return carry

    lax.fori_loop(1, cols, add_every, 0)


def place_kernel(keys_ref, values_ref, total_ref, out_ref, occupancy_ref, *rest):
    accs, (outbuf, sems) = rest[:CHAINS], rest[CHAINS:]
    step = pl.program_id(0)
    sources, _, capacity = keys_ref.shape
    cells = accs[0].shape[0] - SUB
    tiles = cells // ROWS_DEV

    @pl.when(step == 0)
    def _():
        occupancy_ref[...] = total_ref[:, :tiles]
        for acc in accs:
            acc[...] = jnp.zeros_like(acc)

    def source(s, carry):
        row = pl.multiple_of(s * capacity, capacity)
        for j in range(0, capacity, CHAINS):
            at = [keys_ref[s, 0, j + q] for q in range(CHAINS)]
            sums = [
                accs[q][pl.ds(at[q], 1), :] + values_ref[pl.ds(row + j + q, 1), :]
                for q in range(CHAINS)
            ]
            for q in range(CHAINS):
                accs[q][pl.ds(at[q], 1), :] = sums[q]
        return carry

    lax.fori_loop(0, sources, source, 0)

    @pl.when(step == pl.num_programs(0) - 1)
    def _():
        copies = []
        for g in range(ROWS_DEV // SUB):
            for c in range(tiles):
                at = pl.ds((g * tiles + c) * SUB, SUB)
                total = accs[0][at, :]
                for acc in accs[1:]:
                    total = total + acc[at, :]
                outbuf[g * SUB : (g + 1) * SUB, c * TILE : (c + 1) * TILE] = total
            rows = pl.ds(g * SUB, SUB)
            copy = pltpu.make_async_copy(outbuf.at[rows], out_ref.at[rows], sems.at[g])
            copy.start()
            copies.append(copy)
        for copy in copies:
            copy.wait()


def body(block_values, block_owner, block_offset, block_tiles):
    tiles_count = F // TILE
    size_row = lax.axis_size("row")
    size_col = lax.axis_size("col")
    devices_all = size_row * size_col
    local_blocks = block_values.shape[0]
    capacity = 2 * local_blocks // devices_all
    slots_total = devices_all * capacity
    owner = block_owner[:, 0]
    cells = ROWS_DEV * tiles_count
    owner_hot = (owner[:, None] == jnp.arange(devices_all, dtype=jnp.int32)[None, :]).astype(
        jnp.bfloat16
    )
    positions = jnp.arange(local_blocks, dtype=jnp.int32)
    earlier = (positions[None, :] < positions[:, None]).astype(jnp.bfloat16)
    before = jnp.dot(earlier, owner_hot, preferred_element_type=jnp.float32)
    slot = jnp.sum(before * owner_hot.astype(jnp.float32), axis=1).astype(jnp.int32)
    target = owner * capacity + slot
    local_keys = (block_offset // SUB * tiles_count + block_tiles) * SUB + block_offset % SUB

    vmem, smem, anywhere = (
        pl.BlockSpec(memory_space=m) for m in (pltpu.VMEM, pltpu.SMEM, pl.ANY)
    )
    fill = jnp.full((slots_total,), cells, jnp.int32)
    send, send_keys = pl.pallas_call(
        spread_kernel,
        out_shape=(
            jax.ShapeDtypeStruct((slots_total, TILE), jnp.float32),
            jax.ShapeDtypeStruct((slots_total,), jnp.int32),
        ),
        in_specs=[smem, smem, anywhere, vmem],
        out_specs=(vmem, smem),
        scratch_shapes=[pltpu.SemaphoreType.DMA],
        name="spread",
    )(target, local_keys, fill, block_values)

    rows_total = ROWS_DEV * devices_all
    tile_rows = rows_total // TILE
    block_row = owner * ROWS_DEV + block_offset
    tile_row = block_row // TILE
    row_hot = (jnp.arange(tile_rows, dtype=jnp.int32)[:, None] == tile_row[None, :]).astype(
        jnp.bfloat16
    )
    col_hot = (jnp.arange(TILE, dtype=jnp.int32)[:, None] == block_tiles[None, :]).astype(
        jnp.bfloat16
    )
    local_counts = lax.dot_general(
        row_hot, col_hot, (((1,), (1,)), ((), ())), preferred_element_type=jnp.float32
    ).astype(jnp.int32)

    sems = pltpu.SemaphoreType.DMA
    got, got_keys, total = pl.pallas_call(
        functools.partial(exchange_kernel, size_row, size_col),
        out_shape=(
            jax.ShapeDtypeStruct((devices_all, capacity, TILE), jnp.float32),
            jax.ShapeDtypeStruct((devices_all, 1, capacity), jnp.int32),
            jax.ShapeDtypeStruct((tile_rows, TILE), jnp.int32),
        ),
        in_specs=[anywhere, anywhere, anywhere],
        out_specs=(anywhere, anywhere, vmem),
        scratch_shapes=[
            pltpu.VMEM((size_row, tile_rows, TILE), jnp.int32),
            pltpu.VMEM((size_col, size_row, tile_rows, TILE), jnp.int32),
            pltpu.VMEM((capacity, TILE), jnp.float32),
            sems((devices_all,)),
            sems((devices_all,)),
            sems((devices_all,)),
            sems((devices_all,)),
            sems((size_row,)),
            sems((size_row,)),
            sems((size_col,)),
            sems((size_col,)),
            sems((3,)),
        ],
        compiler_params=pltpu.CompilerParams(collective_id=0, has_side_effects=True),
        name="exchange",
    )(
        send.reshape(devices_all, capacity, TILE),
        send_keys.reshape(devices_all, 1, capacity),
        local_counts,
    )

    batch = math.gcd(devices_all, 4)
    summed, occupancy = pl.pallas_call(
        place_kernel,
        out_shape=(
            jax.ShapeDtypeStruct((ROWS_DEV, F), jnp.float32),
            jax.ShapeDtypeStruct((tile_rows, tiles_count), jnp.int32),
        ),
        grid=(devices_all // batch,),
        in_specs=[
            pl.BlockSpec((batch, 1, capacity), lambda i: (i, 0, 0), memory_space=pltpu.SMEM),
            pl.BlockSpec((batch * capacity, TILE), lambda i: (i, 0)),
            vmem,
        ],
        out_specs=(anywhere, vmem),
        scratch_shapes=[pltpu.VMEM((cells + SUB, TILE), jnp.float32)] * CHAINS
        + [pltpu.VMEM((ROWS_DEV, F), jnp.float32), sems((ROWS_DEV // SUB,))],
        name="place",
    )(got_keys, got.reshape(slots_total, TILE), total)
    return (summed, occupancy)


def solution(mesh):
    in_specs = (
        P(("row", "col"), None),
        P(("row", "col"), None),
        P(("row", "col")),
        P(("row", "col")),
    )
    out_specs = (P(("row", "col"), None), P())
    return jax.shard_map(body, mesh=mesh, in_specs=in_specs, out_specs=out_specs, check_vma=False)
```
